256 devices in a mesh: sep: 8 (over x, core), sub: 32 (over z, y).
Axes of the slice: x: 4, y: 4, z: 8, core: 2. Of those that a mesh axis runs over, the one named last changes fastest.
Arguments:
- g_top: bfloat16 [2048, 2048], P('sub', 'sep'), may hold values from -8 to 32, as said below
- u_mid: bfloat16 [8, 2048, 512], P('sep', 'sub'), may hold values from -0.125 to 0.125
- b_mid: float32 [8, 512, 512], P('sep', 'sub'), may hold values from -8 to 32
- u_leaf: bfloat16 [256, 1536, 1536], P(('sep', 'sub')), may hold values from -0.15625 to 0.15625
- leaf_index: int32 [256, 1536], P(('sep', 'sub')), may hold values from 0 to 2559, as said below
- leaf_count: int32 [256], P(('sep', 'sub')), may hold values from 768 to 1536, as said below
- leaf_bdiag: float32 [256, 1536], P(('sep', 'sub')), may hold values from 4 to 16
Outputs:
- mid_cross: bfloat16 [8, 2048, 512], P('sep', 'sub')
- mid_block: bfloat16 [8, 512, 512], P('sep', 'sub')
- leaf_offdiag: bfloat16 [256, 1536, 1536], P(('sep', 'sub'))
- leaf_diag: float32 [256, 1536], P(('sep', 'sub'))
The draws below stay inside these ranges and needn't reach their ends.
Inputs may be any that keep to these rules, and one draw needn't show every extreme that they name: g_top is symmetric. `leaf_index`: A leaf's 1536 entries are distinct; an entry below 2048 is a row of the top separator, an entry r of 2048 or more is row r - 2048 of the leaf's middle separator. `leaf_count`: some leaf has all 1536 slots live.
All inputs are finite; a program needn't handle non-finite values.
Results may differ from the reference program's by a relative error of at most 0.004.
Values may be sent and summed in bfloat16 or wider, within the bound.
No kernel may reach another device: no remote copies, remote signals or barrier semaphores. Data moves between devices by JAX's collectives and lax.ppermute only.
A program may use at most 128 MiB of HBM per device.

```python
import math
import jax
import jax.numpy as jnp
from jax import lax

NT = 2048
NM = 512
BORDER = 1536
LEAF_COLS = 1536
MIDS = 8
LEAVES = 256
N_SUB = 32


def symmetric_draw(member_key, order):
    spread_key, diagonal_key = jax.random.split(member_key)
    spread = jnp.clip(jax.random.normal(spread_key, (order, order), jnp.float32), -3.0, 3.0)
    coupling = (spread + spread.T) * (4.0 / math.sqrt(order))
    diagonal = jax.random.uniform(diagonal_key, (order,), jnp.float32, 8.0, 32.0)
    return jnp.where(jnp.eye(order, dtype=bool), jnp.diag(diagonal), coupling)


def draw_g_top(key, part):
    return symmetric_draw(jax.random.fold_in(key, 11), NT).astype(jnp.bfloat16)


def draw_b_mid(key, part):
    member_keys = jax.random.split(jax.random.fold_in(key, 23), MIDS)
    return jax.vmap(lambda member_key: symmetric_draw(member_key, NM))(member_keys)


def draw_leaf_index(key, part):
    member_keys = jax.random.split(jax.random.fold_in(key, 37), LEAVES)

    def ordering(member_key):
        return jax.random.permutation(member_key, NT + NM)[:BORDER].astype(jnp.int32)
    return jax.vmap(ordering)(member_keys)


def draw_leaf_count(key, part):
    count_key, pick_key = jax.random.split(jax.random.fold_in(key, 41))
    counts = jax.random.randint(count_key, (LEAVES,), BORDER // 2, BORDER + 1, dtype=jnp.int32)
    fullest = jax.random.randint(pick_key, (), 0, LEAVES, dtype=jnp.int32)
    positions = jnp.arange(LEAVES, dtype=jnp.int32)
    return jnp.where(positions == fullest, jnp.int32(BORDER), counts).astype(jnp.int32)


def levels(stream_key, extent, cuts, least, top_value):
    def one(position, shards_of):
        heights = jax.random.uniform(jax.random.fold_in(jax.random.fold_in(stream_key, 6), position), (shards_of,), jnp.float32, least / len(cuts), top_value / len(cuts))
        return jnp.repeat(jnp.exp(heights), extent[position] // shards_of).reshape((-1,) + (1,) * (len(extent) - position - 1))

    loudness = one(*cuts[0])
    for cut in cuts[1:]:
        loudness = loudness * one(*cut)
    return loudness


def gaussian(rng, dims, scale, reach, pieces=(), kind=jnp.bfloat16):
    result = scale * jax.random.normal(rng, dims, jnp.float32)
    if pieces:
        result = result * levels(rng, dims, pieces, -0.22, 0.18)
    return jnp.clip(result, -reach, reach).astype(kind)


def setup_inputs(seed: int = 0) -> dict:
    splits = jax.random.split(jax.random.key(seed), 8)
    g_top = draw_g_top(jax.random.fold_in(splits[7], 71), 0)
    u_mid = gaussian(splits[1], (MIDS, NT, NM), NT ** -0.5, 0.125, ((0, 8), (1, 32)))
    b_mid = draw_b_mid(jax.random.fold_in(splits[7], 71), 0)
    u_leaf = gaussian(splits[3], (LEAVES, BORDER, LEAF_COLS), BORDER ** -0.5, 0.15625, ((0, 256),))
    leaf_index = draw_leaf_index(jax.random.fold_in(splits[7], 71), 0)
    leaf_count = draw_leaf_count(jax.random.fold_in(splits[7], 71), 0)
    leaf_bdiag = jnp.clip(4.0 + 12.0 * jax.random.uniform(splits[6], (LEAVES, LEAF_COLS), jnp.float32) ** levels(splits[6], (LEAVES, LEAF_COLS), ((0, 256),), -0.2, 0.2), 4.0, 16.0)
    return dict(g_top=g_top, u_mid=u_mid, b_mid=b_mid, u_leaf=u_leaf, leaf_index=leaf_index, leaf_count=leaf_count, leaf_bdiag=leaf_bdiag)


def reference(g_top, u_mid, b_mid, u_leaf, leaf_index, leaf_count, leaf_bdiag):
    def middle(operands):
        factor, inverse_block = operands
        cross_rows = (-jnp.dot(g_top, factor, preferred_element_type=jnp.float32)).astype(jnp.bfloat16)
        projected = jnp.dot(factor.T, cross_rows, preferred_element_type=jnp.float32)
        mid_rows = (inverse_block - projected).astype(jnp.bfloat16)
        return cross_rows, mid_rows

    mid_cross, mid_block = lax.map(middle, (u_mid, b_mid))

    def one_leaf(operands):
        owner_group, factor, slot_index, live_count, bdiagonal = operands
        cross_rows = mid_cross[owner_group]
        mid_rows = mid_block[owner_group]
        upper_rows = jnp.concatenate([g_top, cross_rows], axis=1)
        top_side = slot_index < NT
        clipped = jnp.minimum(slot_index, NT - 1).astype(jnp.int32)
        midpos = jnp.maximum(slot_index - NT, 0).astype(jnp.int32)
        picked = jnp.take(jnp.take(upper_rows, clipped, axis=0), slot_index, axis=1)
        mid_mid = jnp.take(jnp.take(mid_rows, midpos, axis=0), midpos, axis=1)
        chosen = jnp.where(top_side[:, None], picked, jnp.where(top_side[None, :], picked.T, mid_mid))
        live_slot = jnp.arange(BORDER, dtype=jnp.int32) < live_count
        masked = jnp.where(live_slot[:, None], factor, jnp.zeros((), factor.dtype))
        product = jnp.dot(chosen, masked, preferred_element_type=jnp.float32)
        offdiag = jnp.where(live_slot[:, None], -product, jnp.zeros((), jnp.float32)).astype(jnp.bfloat16)
        diagonal = bdiagonal + jnp.sum(masked.astype(jnp.float32) * product, axis=0)
        return offdiag, diagonal

    groups = (jnp.arange(LEAVES, dtype=jnp.int32) // N_SUB).astype(jnp.int32)
    leaf_offdiag, leaf_diag = lax.map(one_leaf, (groups, u_leaf, leaf_index, leaf_count, leaf_bdiag))
    return mid_cross, mid_block, leaf_offdiag, leaf_diag
```

```python
import jax
import jax.numpy as jnp
from jax import lax
from jax.experimental import pallas as pl
from jax.experimental.pallas import tpu as pltpu
from jax.sharding import Mesh
from jax.sharding import PartitionSpec as P

BORDER=1536; COLS=1536; NT=2048; NM=512; ALL=2560; LB=12
SU=1544; SW=2568

def scatter_body(idx_ref, cnt_ref, u_ref, w_ref, uf, wf):
    cnt=cnt_ref[0]
    wf[...] = jnp.zeros(wf.shape, jnp.float32)
    for c in range(LB):
        uf[c*SU:c*SU+BORDER,:] = u_ref[:, c*128:(c+1)*128].astype(jnp.float32)
    def step(i, _):
        base=i*8
        for j in range(8):
            k=base+j
            r=jnp.where(k<cnt, idx_ref[k], ALL)
            wf[pl.ds(r, LB, stride=SW),:] = uf[pl.ds(k, LB, stride=SU),:]
        return 0
    lax.fori_loop(0, BORDER//8, step, 0)
    for c in range(LB):
        w_ref[:, c*128:(c+1)*128] = wf[c*SW:c*SW+ALL,:].astype(jnp.bfloat16)

def scatter_rows(idx, cnt, u):
    return pl.pallas_call(
        scatter_body,
        in_specs=[pl.BlockSpec(memory_space=pltpu.SMEM), pl.BlockSpec(memory_space=pltpu.SMEM), pl.BlockSpec(memory_space=pltpu.VMEM)],
        out_specs=pl.BlockSpec(memory_space=pltpu.VMEM),
        out_shape=jax.ShapeDtypeStruct((ALL,COLS), jnp.bfloat16),
        scratch_shapes=[pltpu.VMEM((LB*SU,128),jnp.float32), pltpu.VMEM((LB*SW,128),jnp.float32)],
        compiler_params=pltpu.CompilerParams(vmem_limit_bytes=60*1024*1024),
        name="scatter_rows",
    )(idx, cnt, u)

VL=60*1024*1024
HBM=pl.BlockSpec(memory_space=pl.ANY)
SM=pl.BlockSpec(memory_space=pltpu.SMEM)
VM=pl.BlockSpec(memory_space=pltpu.VMEM)
REL=(0,-1,1,-2,2,-3,3)

def mid_body(pos, *refs):
    pieces=refs[:9]; w_ref=refs[9]
    u_ref, ut_ref, wp_ref, q_ref, dq_ref, u_v, b_v, sem = refs[10:]
    n=pl.program_id(0)
    @pl.when(n==0)
    def _():
        z=pos[0]
        cps=[]
        for i in range(9):
            zz=(z+REL[i]+8)%8 if i<7 else (z+4)%8
            for yy in range(4 if i<7 else 2):
                y=yy+(2 if i==8 else 0)
                r=pl.multiple_of(zz*256+y*64,64); rb=pl.multiple_of(zz*64+y*16,16)
                cps.append(pltpu.make_async_copy(pieces[i].at[yy,pl.ds(0,64),:], u_v.at[pl.ds(r,64),:], sem.at[len(cps)]))
                cps.append(pltpu.make_async_copy(pieces[i].at[yy,pl.ds(64,16),:], b_v.at[pl.ds(rb,16),:], sem.at[len(cps)]))
        for c in cps: c.start()
        for c in cps: c.wait()
        u_ref[...]=u_v[...]
        for m in range(8):
            ut_ref[:, m*256:(m+1)*256]=u_v[m*256:(m+1)*256,:].T
    wm=w_ref[NT:,:]
    for m in range(4):
        s=slice(m*512,(m+1)*512)
        wp_ref[s,:]=(w_ref[s,:].astype(jnp.float32)-jnp.dot(u_v[s,:],wm,preferred_element_type=jnp.float32)).astype(jnp.bfloat16)
    q=jnp.dot(b_v[...],wm,preferred_element_type=jnp.float32)
    q_ref[...]=q
    dq_ref[...]=jnp.sum((wm.astype(jnp.float32)*q).reshape(NM//8,8,q.shape[1]),axis=0)

def mid_stage(pos, pieces, w):
    bn=256
    return pl.pallas_call(
        mid_body, grid=(COLS//bn,),
        in_specs=[SM]+[HBM]*9+[pl.BlockSpec((ALL,bn),lambda n:(0,n))],
        out_specs=[pl.BlockSpec((NT,NM),lambda n:(0,0)),pl.BlockSpec((NM,NT),lambda n:(0,0)),
                   pl.BlockSpec((NT,bn),lambda n:(0,n)),pl.BlockSpec((NM,bn),lambda n:(0,n)),pl.BlockSpec((8,bn),lambda n:(0,n))],
        out_shape=[jax.ShapeDtypeStruct((NT,NM),jnp.bfloat16),jax.ShapeDtypeStruct((NM,NT),jnp.bfloat16),
                   jax.ShapeDtypeStruct((NT,COLS),jnp.bfloat16),jax.ShapeDtypeStruct((NM,COLS),jnp.float32),jax.ShapeDtypeStruct((8,COLS),jnp.float32)],
        scratch_shapes=[pltpu.VMEM((NT,NM),jnp.bfloat16),pltpu.VMEM((NM,NM),jnp.bfloat16),pltpu.SemaphoreType.DMA((64,))],
        compiler_params=pltpu.CompilerParams(vmem_limit_bytes=VL),
        name="mid_stage",
    )(pos,*pieces,w)

CH=256; SO=CH+8
def final_body(pos, idx_ref, cnt_ref, *refs):
    pieces=refs[:10]
    u_h, ut_h, wp_h, q_h, dq_ref, b_ref, bd_ref = refs[10:17]
    cross_ref, mid_ref, off_h, diag_ref = refs[17:21]
    g, wp, pf, pb, u_v, ut_v, q_v, of, ob, gsem, wsem, usem, utsem, qsem, osem = refs[21:]
    x=pos[2]; c=pos[3]; sub=pos[4]
    gc=[]
    for o in range(2):
        cc=c if o==0 else 1-c
        for i,(dx,y0,ny) in enumerate(((0,0,4),(3,0,4),(1,0,4),(2,0,2),(2,2,2))):
            s=((x+dx)%4)*2+cc
            for d in range(5):
                zz=(s+d)%8
                gc.append(pltpu.make_async_copy(pieces[o*5+i].at[:,d],
                    g.at[zz,pl.ds(y0,ny),:,pl.ds(pl.multiple_of(s*256,256),256)], gsem.at[len(gc)]))
    wc=pltpu.make_async_copy(wp_h,wp,wsem)
    uc=pltpu.make_async_copy(u_h,u_v,usem); utc=pltpu.make_async_copy(ut_h,ut_v,utsem)
    qc=pltpu.make_async_copy(q_h,q_v,qsem)
    for t in gc: t.start()
    wc.start(); uc.start(); utc.start(); qc.start()
    for cb in range(LB):
        pf[cb*SW+ALL:cb*SW+ALL+8,:]=jnp.zeros((8,128),jnp.float32)
    for t in gc: t.wait()
    for s in range(8):
        for d in range(1,4):
            zz=(s+d)%8
            g[s,:,:,zz*256:(zz+1)*256]=g[zz,:,:,s*256:(s+1)*256].reshape(256,256).T.reshape(4,64,256)
    wc.wait()
    def block(m,dg):
        acc=jnp.dot(g[m].reshape(256,NT),wp[...],preferred_element_type=jnp.float32)
        r0=pl.multiple_of(m*256,256)
        pb[pl.ds(r0,256),:]=acc.astype(jnp.bfloat16)
        for cb in range(LB):
            pf[pl.ds(pl.multiple_of(cb*SW+r0,8),256),:]=acc[:,cb*128:(cb+1)*128]
        return dg+jnp.sum((acc*wp[pl.ds(r0,256),:].astype(jnp.float32)).reshape(32,8,COLS),axis=0)
    dg=lax.fori_loop(0,8,block,dq_ref[...])
    diag_ref[...]=bd_ref[...]+jnp.sum(dg,axis=0,keepdims=True)
    uc.wait(); utc.wait(); qc.wait()
    for m in range(2):
        s=slice(m*256,(m+1)*256)
        bot=q_v[s,:]-jnp.dot(ut_v[s,:],pb[...],preferred_element_type=jnp.float32)
        for cb in range(LB):
            pf[cb*SW+NT+m*256:cb*SW+NT+(m+1)*256,:]=bot[:,cb*128:(cb+1)*128]
    own=g[sub//4,sub%4]
    cross_ref[...]=(-jnp.dot(own,u_v[...],preferred_element_type=jnp.float32)).astype(jnp.bfloat16)
    t=jnp.dot(ut_v[pl.ds(pl.multiple_of(sub*16,16),16),:],g[...].reshape(NT,NT),preferred_element_type=jnp.float32)
    hi=t.astype(jnp.bfloat16); lo=(t-hi.astype(jnp.float32)).astype(jnp.bfloat16)
    mid_ref[...]=(b_ref[...]+(jnp.dot(hi,u_v[...],preferred_element_type=jnp.float32)+jnp.dot(lo,u_v[...],preferred_element_type=jnp.float32))).astype(jnp.bfloat16)
    cnt=cnt_ref[0]
    oc=[]
    for ch in range(BORDER//CH):
        def step(i,_,ch=ch):
            for j in range(8):
                k=i*8+j; kk=ch*CH+k
                r=jnp.where(kk<cnt, idx_ref[kk], ALL)
                of[pl.ds(k,LB,stride=SO),:]=pf[pl.ds(r,LB,stride=SW),:]
            return 0
        lax.fori_loop(0,CH//8,step,0)
        sl=ch%2
        if ch>=2: oc[ch-2].wait()
        for cb in range(LB):
            ob[sl,:,cb*128:(cb+1)*128]=(-of[cb*SO:cb*SO+CH,:]).astype(jnp.bfloat16)
        cp=pltpu.make_async_copy(ob.at[sl],off_h.at[pl.ds(ch*CH,CH),:],osem.at[sl])
        cp.start(); oc.append(cp)
    for cp in oc[-2:]: cp.wait()

def final_stage(pos, idx, cnt, pieces, u, ut, wp, q, dq, b_own, bd):
    return pl.pallas_call(
        final_body,
        in_specs=[SM,SM,SM]+[HBM]*10+[HBM]*4+[VM]*3,
        out_specs=[VM,VM,HBM,VM],
        out_shape=[jax.ShapeDtypeStruct((64,NM),jnp.bfloat16),jax.ShapeDtypeStruct((16,NM),jnp.bfloat16),
                   jax.ShapeDtypeStruct((BORDER,COLS),jnp.bfloat16),jax.ShapeDtypeStruct((1,COLS),jnp.float32)],
        scratch_shapes=[pltpu.VMEM((8,4,64,NT),jnp.bfloat16),pltpu.VMEM((NT,COLS),jnp.bfloat16),pltpu.VMEM((LB*SW,128),jnp.float32),
                        pltpu.VMEM((NT,COLS),jnp.bfloat16),pltpu.VMEM((NT,NM),jnp.bfloat16),pltpu.VMEM((NM,NT),jnp.bfloat16),
                        pltpu.VMEM((NM,COLS),jnp.float32),pltpu.VMEM((LB*SO,128),jnp.float32),pltpu.VMEM((2,CH,COLS),jnp.bfloat16),
                        pltpu.SemaphoreType.DMA((50,)),pltpu.SemaphoreType.DMA,pltpu.SemaphoreType.DMA,pltpu.SemaphoreType.DMA,pltpu.SemaphoreType.DMA,pltpu.SemaphoreType.DMA((2,))],
        compiler_params=pltpu.CompilerParams(vmem_limit_bytes=VL),
        name="final_stage",
    )(pos,idx,cnt,*pieces,u,ut,wp,q,dq,b_own,bd)

SIZES={"x":4,"c":2,"z":8,"y":4}
def sh(a, ax, k):
    n=SIZES[ax]
    return lax.ppermute(a, ax, [(i,(i+k)%n) for i in range(n)])
def put(buf, part, i):
    return lax.dynamic_update_slice(buf, part[None], (i,)+(0,)*part.ndim)
def gather_y(part):
    y=lax.axis_index("y")
    r={0:part}
    r[1]=sh(part,"y",1); r[3]=sh(part,"y",-1); r[2]=sh(part,"y",2)
    buf=jnp.zeros((4,)+part.shape,part.dtype)
    for k in range(4):
        buf=put(buf,r[k],(y-k)%4)
    return buf
def comm_g(g):
    z=lax.axis_index("z"); s=2*lax.axis_index("x")+lax.axis_index("c")
    gz=lax.all_to_all(jnp.broadcast_to(g[None],(8,64,256)),"z",0,0,tiled=True)
    sel=lax.dynamic_slice(jnp.concatenate([gz,gz],0),(s,0,0),(5,64,256))
    own=gather_y(sel)
    m1=sh(own,"x",1); p1=sh(own,"x",-1)
    own_o=sh(own,"c",1)
    lo=sh(m1[:2],"x",1); hi=sh(p1[2:],"x",-1)
    m1_o=sh(m1,"c",1); p1_o=sh(p1,"c",1)
    lo_o=sh(lo,"c",1); hi_o=sh(hi,"c",1)
    return (own,m1,p1,lo,hi),(own_o,m1_o,p1_o,lo_o,hi_o)
def comm_u(ub):
    uy=gather_y(ub)
    f=uy; b=uy; out=[uy]
    for t in range(1,4):
        f=sh(f,"z",1); b=sh(b,"z",-1)
        out+=[f,b]
    out+=[sh(f[:2],"z",1), sh(b[2:],"z",-1)]
    return out

def shards(g_top, u_mid, b_mid, u_leaf, leaf_index, leaf_count, leaf_bdiag):
    x, c, z, y = (lax.axis_index(a) for a in ("x", "c", "z", "y"))
    pos = jnp.stack([z, y, x, c, z * 4 + y]).astype(jnp.int32)
    own, other = comm_g(g_top)
    pieces = comm_u(jnp.concatenate([u_mid[0], b_mid[0].astype(jnp.bfloat16)], axis=0))
    w = scatter_rows(leaf_index[0], leaf_count, u_leaf[0])
    u, ut, wp, q, dq = mid_stage(pos, pieces, w)
    cross, mid, off, diag = final_stage(
        pos, leaf_index[0], leaf_count, [*own, *other], u, ut, wp, q, dq, b_mid[0], leaf_bdiag
    )
    return cross[None], mid[None], off[None], diag


def solution(mesh):
    finer = Mesh(mesh.devices.reshape(4, 2, 8, 4), ("x", "c", "z", "y"))
    sep, sub = ("x", "c"), ("z", "y")
    leaf = sep + sub
    return jax.shard_map(
        shards,
        mesh=finer,
        in_specs=(P(sub, sep), P(sep, sub, None), P(sep, sub, None), P(leaf, None, None), P(leaf, None), P(leaf), P(leaf, None)),
        out_specs=(P(sep, sub, None), P(sep, sub, None), P(leaf, None, None), P(leaf, None)),
        check_vma=False,
    )
```
